32 devices in a mesh: groups: 1, tok: 32 (over z, y, x, core).
Axes of the slice: x: 2, y: 2, z: 4, core: 2. Of those that a mesh axis runs over, the one named last changes fastest.
Arguments:
- queries: bfloat16 [4096, 2560], P(('groups', 'tok')), may hold values from -5 to 5
- key_rows: bfloat16 [4096, 2560], P(('groups', 'tok')), may hold values from -5 to 5
- value_rows: bfloat16 [4096, 2560], P(('groups', 'tok')), may hold values from -6 to 6
- learn_rates: float32 [4096, 8], P(('groups', 'tok')), may hold values from 0.0002 to 0.002
- frame_order: int32 [4096], P('groups'), may hold values from 0 to 4095, as said below
- window_ids: int32 [4096], P('groups'), may hold values from 0 to 7, never falling along the last dimension, each value on 1 to 2048 neighbouring positions
- fast_init: bfloat16 [640, 3, 2560], replicated, may hold values from -0.3125 to 0.3125
- norm_gain: float32 [2560], replicated, may hold values from 0.5 to 1.5
Outputs:
- layer_out: bfloat16 [4096, 2560], P(('groups', 'tok'))
The draws below stay inside these ranges and needn't reach their ends.
Inputs may be any that keep to these rules, and one draw needn't show every extreme that they name: frame_order[i] is the sequence position of the token stored at row i; every position appears once, and every aligned block of 128 stored rows holds exactly 4 positions of every aligned block of 128 positions.
All inputs are finite; a program needn't handle non-finite values.
Results may differ from the reference program's by a relative error of at most 0.025.
Values may be sent and summed in bfloat16 or wider, within the bound.
A program may use at most 192 MiB of HBM per device.

```python
import math
import jax
import jax.numpy as jnp
import numpy as np
from jax import lax

HEADS = 8
HEAD_DIM = 320
FAST_HID = 640
ATT_DIM = 128
WINDOW = 1024
TOK_DEV = 128
WIDTH = 2560
ATT_HEADS = 20
TOKENS = 4096
SLOTS = 4


def shuffled(sub_key):
    return jax.random.permutation(sub_key, TOK_DEV)


def make_order(key):
    base = jax.random.fold_in(key, 101)
    sources = TOKENS // TOK_DEV
    send_slots = jax.vmap(shuffled)(jax.random.split(jax.random.fold_in(base, 1), sources))
    recv_slots = jax.vmap(shuffled)(jax.random.split(jax.random.fold_in(base, 2), sources))
    source = jnp.arange(sources, dtype=jnp.int32)[:, None]
    target = send_slots // SLOTS
    within = send_slots % SLOTS
    landing = recv_slots[target, source * SLOTS + within]
    return (target * TOK_DEV + landing).reshape(-1).astype(jnp.int32)


def sequence_rows(key, salt):
    noise_key = jax.random.fold_in(key, salt)
    return jnp.clip(jax.random.normal(noise_key, (TOKENS, WIDTH), jnp.float32), -5.0, 5.0)


def draw_frame_order(key, part):
    return make_order(key)


def draw_queries(key, part):
    rows = sequence_rows(key, 202)
    return rows[make_order(key)].astype(jnp.bfloat16)


def draw_key_rows(key, part):
    rows = sequence_rows(key, 404)
    return rows[make_order(key)].astype(jnp.bfloat16)


def steps_of(own_key, dims, cuts, least, largest):
    level, own = 1.0, jax.random.fold_in(own_key, 6)
    for position, blocks in cuts:
        steps = jnp.exp(jax.random.uniform(jax.random.fold_in(own, position), (blocks,), jnp.float32, least / len(cuts), largest / len(cuts)))
        level = level * jnp.repeat(steps, dims[position] // blocks).reshape([-1 if axis == position else 1 for axis in range(len(dims))])
    return level


def split_up(count, total, bound, slope):
    loads = [(1 << 20) // math.isqrt(rank ** slope) + 1 for rank in range(2, count + 1)]
    surplus, given = total - bound - (count - 1), [1] * (count - 1)
    while surplus > 0:
        movable = [i for i in range(count - 1) if given[i] < bound]
        pool, left = sum([loads[i] for i in movable]), surplus
        for i in movable:
            more = min(bound - given[i], max(1, left * loads[i] // pool), surplus)
            given[i] = given[i] + more
            surplus = surplus - more
    return np.array([bound] + given)


def ragged_sizes(stream_key, count, total, most, slope):
    if count == 2:
        one = jax.random.randint(stream_key, (), max(1, total - most), min(most, total - 1) + 1)
        return jnp.stack([one, total - one])
    sizes = jnp.asarray(split_up(count, total, most, slope), jnp.int32)
    twos = (count - 1) // 2
    giver, receiver = sizes[1:1 + 2 * twos:2], sizes[2:2 + 2 * twos:2]
    slack = jnp.minimum(giver - 1, most - receiver)
    passed = jax.random.randint(jax.random.fold_in(stream_key, 1), (twos,), 0, 1 << 20) % (slack + 1)
    sizes = sizes.at[1:1 + 2 * twos:2].set(giver - passed).at[2:2 + 2 * twos:2].set(receiver + passed)
    return sizes[jax.random.permutation(jax.random.fold_in(stream_key, 2), count)]


def normal_values(stream_key, dims, width, bound, pieces=(), kind=jnp.bfloat16):
    values = width * jax.random.normal(stream_key, dims, jnp.float32)
    if pieces:
        values = values * steps_of(stream_key, dims, pieces, -0.22, 0.18)
    return jnp.clip(values, -bound, bound).astype(kind)


def setup_inputs(seed: int = 0, part: int = 0) -> dict:
    splits = jax.random.split(jax.random.key(seed), 9)
    part_keys = jax.random.split(jax.random.fold_in(splits[8], part), 9)
    queries = draw_queries(jax.random.fold_in(jax.random.fold_in(splits[8], part), 71), part)
    key_rows = draw_key_rows(jax.random.fold_in(jax.random.fold_in(splits[8], part), 71), part)
    value_rows = normal_values(part_keys[2], (TOKENS, WIDTH), 1.0, 6.0, ((0, 32),))
    learn_rates = jnp.clip(jnp.exp(math.log(0.002) - 2.3025852 * jax.random.uniform(part_keys[3], (TOKENS, HEADS), jnp.float32) ** steps_of(part_keys[3], (TOKENS, HEADS), ((0, 32),), -0.2, 0.2)), 0.0002, 0.002)
    frame_order = draw_frame_order(jax.random.fold_in(jax.random.fold_in(splits[8], part), 71), part)
    window_ids = jnp.searchsorted(jnp.cumsum(ragged_sizes(part_keys[5], TOKENS // (WINDOW // 2), TOKENS, 2 * WINDOW, 1)), jnp.arange(TOKENS), side="right").astype(jnp.int32)
    fast_init = normal_values(splits[6], (FAST_HID, 3, WIDTH), HEAD_DIM ** -0.5, 0.3125)
    norm_gain = jnp.clip(1.0 + 0.1 * jax.random.normal(splits[7], (WIDTH,), jnp.float32), 0.5, 1.5)
    return {"queries": queries, "key_rows": key_rows, "value_rows": value_rows, "learn_rates": learn_rates, "frame_order": frame_order, "window_ids": window_ids, "fast_init": fast_init, "norm_gain": norm_gain}


epsilon = 1e-06

def rounded(values):
    return lax.optimization_barrier(values.astype(jnp.bfloat16)).astype(jnp.float32)

def head_view(rows):
    return rows.astype(jnp.float32).reshape(rows.shape[0], HEADS, HEAD_DIM)

def matrix_view(weight_rows, which):
    return weight_rows[:, which].astype(jnp.float32).reshape(weight_rows.shape[0], HEADS, HEAD_DIM)

def fast_grads(key_block, value_block, rate_block, weight_rows):
    row_count = weight_rows.shape[0]
    key_heads = head_view(key_block)
    target = rounded(head_view(value_block) * rate_block.astype(jnp.float32)[:, :, None])
    gate = jnp.einsum('thd,jhd->thj', key_heads, matrix_view(weight_rows, 0))
    upward = jnp.einsum('thd,jhd->thj', key_heads, matrix_view(weight_rows, 1))
    backward = jnp.einsum('thd,jhd->thj', target, matrix_view(weight_rows, 2))
    sigmoid = jax.nn.sigmoid(gate)
    active = gate * sigmoid
    product = rounded(active * upward)
    delta_gate = rounded(backward * upward * sigmoid * (1.0 + gate * (1.0 - sigmoid)))
    delta_upper = rounded(backward * active)
    grad_gate = jnp.einsum('thj,thd->jhd', delta_gate, key_heads)
    grad_upper = jnp.einsum('thj,thd->jhd', delta_upper, key_heads)
    grad_down = jnp.einsum('thj,thd->jhd', product, target)
    return jnp.stack([grad_gate.reshape(row_count, WIDTH), grad_upper.reshape(row_count, WIDTH), grad_down.reshape(row_count, WIDTH)], axis=1)

def renormed(base_rows, grads):
    start_rows = base_rows.astype(jnp.float32)
    update = start_rows + grads
    shaped = update.reshape(update.shape[0], 3, HEADS, HEAD_DIM)
    anchor = start_rows.reshape(update.shape[0], 3, HEADS, HEAD_DIM)
    scaling = jnp.sqrt(lax.optimization_barrier(jnp.sum(anchor * anchor, axis=-1, keepdims=True)) + epsilon) / jnp.sqrt(lax.optimization_barrier(jnp.sum(shaped * shaped, axis=-1, keepdims=True)) + epsilon)
    return (shaped * scaling).reshape(update.shape).astype(jnp.bfloat16)

def fast_apply(query_block, weight_rows):
    query_heads = head_view(query_block)
    gate = jnp.einsum('thd,jhd->thj', query_heads, matrix_view(weight_rows, 0))
    upward = jnp.einsum('thd,jhd->thj', query_heads, matrix_view(weight_rows, 1))
    product = rounded(jax.nn.silu(gate) * upward)
    result = jnp.einsum('thj,jhd->thd', product, matrix_view(weight_rows, 2))
    return result.reshape(query_block.shape[0], WIDTH)

def reference(queries, key_rows, value_rows, learn_rates, frame_order, window_ids, fast_init, norm_gain):
    block_count = TOKENS // TOK_DEV
    indices = jnp.arange(block_count, dtype=jnp.int32)

    def accumulate(total, index):
        begin = index * TOK_DEV
        partial_value = fast_grads(lax.dynamic_slice_in_dim(key_rows, begin, TOK_DEV, 0), lax.dynamic_slice_in_dim(value_rows, begin, TOK_DEV, 0), lax.dynamic_slice_in_dim(learn_rates, begin, TOK_DEV, 0), fast_init)
        return (total + rounded(partial_value), jnp.zeros((), jnp.float32))
    grads = lax.scan(accumulate, jnp.zeros((FAST_HID, 3, WIDTH), jnp.float32), indices)[0]
    fresh = renormed(fast_init, grads)
    query_seq = jnp.zeros_like(queries).at[frame_order].set(queries)
    key_seq = jnp.zeros_like(key_rows).at[frame_order].set(key_rows)
    value_seq = jnp.zeros_like(value_rows).at[frame_order].set(value_rows)

    def apply_block(index):
        return fast_apply(lax.dynamic_slice_in_dim(query_seq, index * TOK_DEV, TOK_DEV, 0), fresh)
    fast_out = lax.map(apply_block, indices).reshape(TOKENS, WIDTH)
    half_span = WINDOW // 2
    span = TOK_DEV + 2 * half_span
    key_pad = jnp.pad(key_seq, ((half_span, half_span), (0, 0)))
    value_pad = jnp.pad(value_seq, ((half_span, half_span), (0, 0)))
    ids_pad = jnp.pad(window_ids, (half_span, half_span), constant_values=-1)

    def attend(index):
        begin = index * TOK_DEV
        query_block = lax.dynamic_slice_in_dim(query_seq, begin, TOK_DEV, 0).astype(jnp.float32).reshape(TOK_DEV, ATT_HEADS, ATT_DIM)
        key_block = lax.dynamic_slice_in_dim(key_pad, begin, span, 0).astype(jnp.float32).reshape(span, ATT_HEADS, ATT_DIM)
        value_block = lax.dynamic_slice_in_dim(value_pad, begin, span, 0).astype(jnp.float32).reshape(span, ATT_HEADS, ATT_DIM)
        query_ids = lax.dynamic_slice_in_dim(window_ids, begin, TOK_DEV, 0)
        key_ids = lax.dynamic_slice_in_dim(ids_pad, begin, span, 0)
        query_pos = begin + jnp.arange(TOK_DEV, dtype=jnp.int32)
        key_pos = begin - half_span + jnp.arange(span, dtype=jnp.int32)
        allowed = (key_pos[None, :] >= 0) & (key_pos[None, :] < TOKENS) & (jnp.abs(query_pos[:, None] - key_pos[None, :]) < half_span) & (query_ids[:, None] == key_ids[None, :])
        scores = jnp.einsum('tad,sad->ats', query_block, key_block) * ATT_DIM ** (-0.5)
        scores = jnp.where(allowed[None], scores, -1e+30)
        peak = lax.optimization_barrier(jnp.max(scores, axis=2, keepdims=True))
        weights = jnp.exp(scores - peak)
        total = lax.optimization_barrier(jnp.sum(weights, axis=2, keepdims=True))
        mixed = jnp.einsum('ats,sad->tad', rounded(weights), value_block)
        return (mixed / jnp.transpose(total, (1, 0, 2))).reshape(TOK_DEV, WIDTH)
    attended = lax.map(attend, indices).reshape(TOKENS, WIDTH)
    combined = fast_out + attended
    mean_square = lax.optimization_barrier(jnp.mean(combined * combined, axis=1, keepdims=True))
    return (combined * lax.rsqrt(mean_square + epsilon) * norm_gain).astype(jnp.bfloat16)
```

```python
import functools

import jax
import jax.numpy as jnp
from jax import lax
from jax.experimental import pallas as pl
from jax.experimental.pallas import tpu as pltpu
from jax.sharding import PartitionSpec as P

HEADS = 8
ATT_DIM = 128
WINDOW = 1024
SPLIT = 4

epsilon = 1e-06
BF = jnp.bfloat16
F32 = jnp.float32
I32 = jnp.int32
LANES = 128
VM = pl.BlockSpec(memory_space=pltpu.VMEM)
ANY = pl.BlockSpec(memory_space=pl.ANY)
NT = (((1,), (1,)), ((), ()))
TN = (((0,), (0,)), ((), ()))
VMEM_BYTES = 62 * 1024 * 1024


def dot_nt(a, b):
    return lax.dot_general(a, b, NT, preferred_element_type=F32)


def dot_tn(a, b):
    return lax.dot_general(a, b, TN, preferred_element_type=F32)


def dot_nn(a, b):
    return jnp.dot(a, b, preferred_element_type=F32)


def iota(shape, dim):
    return lax.broadcasted_iota(I32, shape, dim)


class Place:
    def __init__(self, count):
        self.count = count
        self.segs = count // SPLIT
        self.chips = self.segs // 2

    def shift(self, hd):
        return ((hd % 2) * 2 + hd // 2) % self.chips

    def seg(self, hd, within):
        chip, core = within // 2, within % 2
        if self.chips == 4:
            step = 2 * (chip // 2) + (chip % 2 + chip // 2) % 2
        else:
            step = chip
        return (step - self.shift(hd) + self.chips) % self.chips * 2 + core

    def rank(self, hd, seg):
        pair, core = seg // 2, seg % 2
        step = (pair + self.shift(hd)) % self.chips
        if self.chips == 4:
            chip = 2 * (step // 2) + (step + step // 2) % 2
        else:
            chip = step
        return hd * self.segs + chip * 2 + core


def pack_kernel(segs, order_ref, rate_ref, query_ref, key_ref, value_ref, kv_ref, q_ref, small_ref):
    me = lax.axis_index("tok")
    tokens, width = key_ref.shape
    home = tokens // segs
    row = order_ref[pl.ds(me, 1), :].astype(F32)
    down, across = iota((tokens, tokens), 0), iota((tokens, tokens), 1)
    same = down == across
    column = jnp.sum(jnp.where(same, row, 0.0), axis=1, keepdims=True)
    span = 1.0 / (SPLIT * tokens)

    def sort_key(place, index):
        return jnp.floor((place + 0.5) * span) * tokens + index.astype(F32)

    key_row = sort_key(row, iota((1, tokens), 1))
    key_column = sort_key(column, iota((tokens, 1), 0))
    rank_row = jnp.sum(jnp.where(key_column < key_row, 1.0, 0.0), axis=0, keepdims=True)
    rank_column = jnp.sum(jnp.where(key_row < key_column, 1.0, 0.0), axis=1, keepdims=True)
    pick = jnp.where(down.astype(F32) == rank_row, 1.0, 0.0).astype(BF)
    keys = dot_nn(pick, key_ref[...]).astype(BF)
    values = dot_nn(pick, value_ref[...]).astype(BF)
    rows = dot_nn(pick, query_ref[...]).astype(BF)
    kv_ref[0, :, 0:home, :] = keys.reshape(segs, home, width)
    kv_ref[0, :, home : 2 * home, :] = values.reshape(segs, home, width)
    q_ref[0] = rows.reshape(segs, home, width)

    @pl.when(pl.program_id(0) == 0)
    def _():
        put = jnp.where(across.astype(F32) == rank_column, 1.0, 0.0)
        place = jnp.sum(put * column, axis=0, keepdims=True)
        rates = jnp.dot(rate_ref[...], put, precision=lax.Precision.HIGHEST)
        heads = HEADS // SPLIT
        for hd in range(SPLIT):
            small_ref[hd, 0:heads, :] = rates[hd * heads : (hd + 1) * heads]
            small_ref[hd, heads : heads + 1, :] = place
            small_ref[hd, heads + 1 :, :] = jnp.zeros_like(small_ref[hd, heads + 1 :, :])


def layer_kernel(
    place, head_dim, kv_ref, q_ref, small_ref, ids_ref, init_ref, gain_ref, out_ref,
    kv, queries, small, weight, total, part, half_in, half, slices, fresh, ahead, sorted_q,
    bias, combined, outgoing, returned,
    init_sem, kv_send, kv_recv, q_send, q_recv, small_send, small_recv, next_send, next_recv,
    prev_send, prev_recv, core_send, core_recv, cut_send, cut_recv, share_send, share_recv,
    pass_send, pass_recv, back_send, back_recv,
):
    me = lax.axis_index("tok")
    count, segs, chips = place.count, place.segs, place.chips
    hd, within = me // segs, me % segs
    chip, core = within // 2, within % 2
    seg = place.seg(hd, within)
    home, width = queries.shape[1], queries.shape[2]
    tokens = count * home
    hidden = weight.shape[1]
    side = hidden // 2
    rows = side // chips
    heads = width // head_dim
    partner = me + 1 - 2 * core
    after = place.rank(hd, (seg + 1) % segs)
    before = place.rank(hd, (seg + segs - 1) % segs)

    def remote(src, dst, send, recv, device):
        return pltpu.make_async_remote_copy(
            src_ref=src, dst_ref=dst, send_sem=send, recv_sem=recv,
            device_id={"tok": device}, device_id_type=pl.DeviceIdType.MESH,
        )

    def wait_all(buffer, sem):
        pltpu.make_async_copy(buffer, buffer, sem).wait()

    columns = pl.ds(pl.multiple_of(hd * width, LANES), width)
    load = pltpu.make_async_copy(init_ref.at[:, :, columns], weight, init_sem)
    load.start()

    barrier = pltpu.get_barrier_semaphore()

    def greet(step, carry):
        pl.semaphore_signal(
            barrier, inc=1, device_id={"tok": (me + step) % count},
            device_id_type=pl.DeviceIdType.MESH,
        )
        return carry

    lax.fori_loop(1, count, greet, 0)
    pl.semaphore_wait(barrier, count - 1)

    planes = [(hd + 2) % 4, 3 - hd, hd + 1 - 2 * (hd % 2), hd]

    def send_rows(plane, first):
        def body(step, carry):
            spot = (within + step) % segs
            there = plane * segs + spot
            where = place.seg(plane, spot)
            remote(small_ref.at[plane], small.at[me], small_send, small_recv, there).start()
            remote(kv_ref.at[plane, where], kv.at[1, me], kv_send, kv_recv.at[me], there).start()
            return carry

        lax.fori_loop(first, segs, body, 0)

    def send_queries(plane, first):
        def body(step, carry):
            spot = (within + step) % segs
            there = plane * segs + spot
            where = place.seg(plane, spot)
            remote(q_ref.at[plane, where], queries.at[me], q_send, q_recv, there).start()
            return carry

        lax.fori_loop(first, segs, body, 0)

    for order, plane in enumerate(planes):
        send_rows(plane, 1 if order == 3 else 0)

    def forward(block, source):
        remote(block, kv.at[0, source], next_send, next_recv, after).start()
        remote(block, kv.at[2, source], prev_send, prev_recv, before).start()

    own = kv_ref.at[hd, seg]
    forward(own, me)
    kv[1, me] = kv_ref[hd, seg]
    queries[me] = q_ref[hd, seg]
    small[me] = small_ref[hd]

    def arrive(plane, first):
        def body(step, carry):
            source = plane * segs + (within + segs - step) % segs
            block = kv.at[1, source]
            remote(block, block, kv_send, kv_recv.at[source], source).wait_recv()
            forward(block, source)
            return carry

        lax.fori_loop(first, segs, body, 0)

    total[...] = jnp.zeros_like(total)

    column = iota((1, width), 1)

    def span(which):
        low = which * head_dim // LANES * LANES
        high = -(-(which + 1) * head_dim // LANES) * LANES
        inside = (column[:, low:high] >= which * head_dim) & (
            column[:, low:high] < (which + 1) * head_dim
        )
        return slice(low, high), inside

    def pick_column(index, base, sources, which):
        lane = iota((home, LANES), 1) == index * home + iota((home, LANES), 0)
        held = small[pl.ds(base, sources), which, :]
        chosen = jnp.where(lane[None], held[:, None, :], 0.0)
        return jnp.sum(chosen, axis=2, keepdims=True).reshape(sources * home, 1)

    def learn(base, sources):
        group = sources * home
        for which in range(heads):
            lanes, inside = span(which)
            keys = kv[1, pl.ds(base, sources), 0:home, lanes].reshape(group, -1)
            values = kv[1, pl.ds(base, sources), home : 2 * home, lanes].reshape(group, -1)
            rate = pick_column(seg, base, sources, which)
            key_part = jnp.where(inside, keys.astype(F32), 0.0).astype(BF)
            target = jnp.where(inside, values.astype(F32) * rate, 0.0).astype(BF)
            gate = dot_nt(key_part, weight[0, :, lanes])
            upward = dot_nt(key_part, weight[1, :, lanes])
            backward = dot_nt(target, weight[2, :, lanes])
            sigmoid = jax.nn.sigmoid(gate)
            active = gate * sigmoid
            product = (active * upward).astype(BF)
            delta_gate = (backward * upward * sigmoid * (1.0 + gate * (1.0 - sigmoid))).astype(BF)
            delta_upper = (backward * active).astype(BF)
            total[0, :, lanes] += dot_tn(delta_gate, key_part)
            total[1, :, lanes] += dot_tn(delta_upper, key_part)
            total[2, :, lanes] += dot_tn(product, target)

    wait_all(small.at[pl.ds(0, count - 1)], small_recv)
    arrive(planes[3], 1)
    arrive(planes[2], 0)
    load.wait()
    near = hd // 2 * 2 * segs
    learn(near, 2 * segs)
    for order, plane in enumerate(planes):
        send_queries(plane, 1 if order == 3 else 0)
    arrive(planes[1], 0)
    arrive(planes[0], 0)
    learn(2 * segs - near, 2 * segs)

    theirs = pl.ds(pl.multiple_of((1 - core) * side, 16), side)
    part[...] = total[:, theirs, :].astype(BF)
    swap = remote(part, half_in, core_send, core_recv, partner)
    swap.start()
    swap.wait_recv()

    def fold(step, carry):
        spot = (chip + 1 + step) % chips
        mine = pl.ds(pl.multiple_of(core * side + spot * rows, 16), rows)
        theirs = pl.ds(pl.multiple_of(spot * rows, 16), rows)
        half[spot] = (total[:, mine, :] + half_in[:, theirs, :].astype(F32)).astype(BF)

        @pl.when(step < chips - 1)
        def _():
            there = hd * segs + spot * 2 + core
            remote(half.at[spot], slices.at[chip], cut_send, cut_recv.at[chip], there).start()

        return carry

    lax.fori_loop(0, chips, fold, 0)

    wait_all(kv.at[0], next_recv)
    wait_all(kv.at[2], prev_recv)

    def order_of(index):
        spot = pick_column(index, 0, count, heads)
        down, across = iota((tokens, tokens), 0), iota((tokens, tokens), 1)
        row = jnp.sum(jnp.where(down == across, spot, 0.0), axis=0, keepdims=True)
        return jnp.where((down + index * tokens).astype(F32) == row, 1.0, 0.0).astype(BF)

    for which, index in enumerate(((seg + segs - 1) % segs, seg, (seg + 1) % segs)):
        sort = order_of(index)
        keys = kv[which, :, 0:home, :].reshape(tokens, width)
        values = kv[which, :, home : 2 * home, :].reshape(tokens, width)
        ahead[0, which * tokens : (which + 1) * tokens, :] = dot_nn(sort, keys).astype(BF)
        ahead[1, which * tokens : (which + 1) * tokens, :] = dot_nn(sort, values).astype(BF)
        if which == 1:
            wait_all(queries.at[pl.ds(0, count - 1)], q_recv)
            sorted_q[...] = dot_nn(sort, queries[...].reshape(tokens, width)).astype(BF)

    reach = WINDOW // 2
    chunk = LANES
    wide = chunk + 2 * reach
    blocks = tokens // chunk
    id_rows = ids_ref.shape[0]
    down, across = iota((chunk, chunk), 0), iota((chunk, chunk), 1)
    for part_index in range(blocks):
        middle = seg * blocks + part_index
        mine = ids_ref[pl.ds(middle, 1), :]
        mine = jnp.sum(jnp.where(down == across, mine, 0), axis=1, keepdims=True)
        for tile in range(wide // chunk):
            block = middle - reach // chunk + tile
            valid = (block >= 0) & (block < id_rows)
            other = ids_ref[pl.ds((block + id_rows) % id_rows, 1), :]
            other = jnp.where(valid, other, -1)
            distance = down - across + (reach - tile * chunk)
            allowed = (mine == other) & (distance < reach) & (distance > -reach)
            bias[part_index, :, tile * chunk : (tile + 1) * chunk] = jnp.where(
                allowed, 0.0, -1e30
            )

    def attend(head, carry):
        lanes = pl.ds(pl.multiple_of(head * ATT_DIM, LANES), ATT_DIM)
        for part_index in range(blocks):
            begin = part_index * chunk
            query = sorted_q[begin : begin + chunk, lanes]
            keys = ahead[0, begin : begin + wide, lanes]
            values = ahead[1, begin : begin + wide, lanes]
            scores = dot_nt(query, keys) * ATT_DIM ** (-0.5) + bias[part_index]
            peak = jnp.max(scores, axis=1, keepdims=True)
            weights = jnp.exp(scores - peak)
            norm = jnp.sum(weights, axis=1, keepdims=True)
            combined[begin : begin + chunk, lanes] = dot_nn(weights.astype(BF), values) / norm
        return carry

    def cut_arrive(step, carry):
        source = (chip + step) % chips
        block = slices.at[source]
        remote(block, block, cut_send, cut_recv.at[source], me).wait_recv()
        return carry

    early = width // ATT_DIM // 2
    lax.fori_loop(0, early, attend, 0)

    lax.fori_loop(1, chips, cut_arrive, 0)
    slices[chip] = half[chip]
    slot = core * chips + chip
    mine = pl.ds(pl.multiple_of(slot * rows, 16), rows)
    for matrix in range(3):
        base = weight[matrix, mine, :].astype(F32)
        update = base + jnp.sum(slices[:, matrix].astype(F32), axis=0)
        scaling = jnp.zeros_like(update)
        for which in range(heads):
            inside = (column >= which * head_dim) & (column < (which + 1) * head_dim)
            old = jnp.sum(jnp.where(inside, base * base, 0.0), axis=1, keepdims=True)
            new = jnp.sum(jnp.where(inside, update * update, 0.0), axis=1, keepdims=True)
            ratio = jnp.sqrt(old + epsilon) / jnp.sqrt(new + epsilon)
            scaling = jnp.where(inside, ratio, scaling)
        fresh[slot, matrix] = (update * scaling).astype(BF)

    def share(step, carry):
        spot = (chip + step) % chips
        there = hd * segs + spot * 2 + core
        remote(fresh.at[slot], fresh.at[slot], share_send, share_recv.at[chip], there).start()
        return carry

    lax.fori_loop(1, chips, share, 0)

    def hand(index):
        remote(fresh.at[index], fresh.at[index], pass_send, pass_recv, partner).start()

    hand(slot)
    lax.fori_loop(early, width // ATT_DIM, attend, 0)

    def shared(step, carry):
        source = (chip + step) % chips
        block = fresh.at[core * chips + source]
        remote(block, block, share_send, share_recv.at[source], me).wait_recv()
        hand(core * chips + source)
        return carry

    lax.fori_loop(1, chips, shared, 0)
    wait_all(fresh.at[pl.ds(0, chips)], pass_recv)

    for which in range(heads):
        lanes, inside = span(which)
        query = jnp.where(inside, sorted_q[:, lanes].astype(F32), 0.0).astype(BF)

        def matrix_of(matrix):
            return fresh[:, matrix, :, lanes].reshape(hidden, -1)

        gate = dot_nt(query, matrix_of(0))
        upward = dot_nt(query, matrix_of(1))
        product = (gate * jax.nn.sigmoid(gate) * upward).astype(BF)
        combined[:, lanes] += jnp.where(inside, dot_nn(product, matrix_of(2)), 0.0)

    tok_dev = out_ref.shape[0]
    for piece in range(SPLIT):
        there = seg * SPLIT + piece
        outgoing[piece] = combined[piece * tok_dev : (piece + 1) * tok_dev, :].astype(BF)

        @pl.when(there != me)
        def _():
            remote(
                outgoing.at[piece], returned.at[hd], back_send.at[piece], back_recv.at[hd], there
            ).start()

        @pl.when(there == me)
        def _():
            returned[hd] = outgoing[piece]

    for source in range(SPLIT):
        block = returned.at[source]

        @pl.when(place.rank(source, me // SPLIT) != me)
        def _():
            remote(block, block, back_send.at[0], back_recv.at[source], me).wait_recv()

    square = 0.0
    for source in range(SPLIT):
        piece = returned[source].astype(F32)
        square = square + jnp.sum(piece * piece, axis=1, keepdims=True)
    scale = lax.rsqrt(square / (SPLIT * width) + epsilon)
    for source in range(SPLIT):
        lanes = slice(source * width, (source + 1) * width)
        out_ref[:, lanes] = (returned[source].astype(F32) * scale * gain_ref[:, lanes]).astype(BF)

    wait_all(small.at[pl.ds(0, count - 1)], small_send)
    wait_all(kv.at[1, pl.ds(0, count - 1)], kv_send)
    wait_all(queries.at[pl.ds(0, count - 1)], q_send)
    wait_all(kv.at[0], next_send)
    wait_all(kv.at[2], prev_send)
    swap.wait_send()
    wait_all(slices.at[pl.ds(0, chips - 1)], cut_send)
    wait_all(fresh.at[pl.ds(0, chips - 1)], share_send)
    wait_all(fresh.at[pl.ds(0, chips)], pass_send)
    for piece in range(SPLIT):
        block = outgoing.at[piece]

        @pl.when(seg * SPLIT + piece != me)
        def _():
            remote(block, block, back_send.at[piece], back_recv.at[0], me).wait_send()


def shards(
    queries, key_rows, value_rows, learn_rates, frame_order, window_ids, fast_init, norm_gain
):
    tok_dev, model = queries.shape
    count = lax.axis_size("tok")
    place = Place(count)
    segs, chips = place.segs, place.chips
    assert count % (2 * SPLIT) == 0 and tok_dev % segs == 0
    home = tok_dev // segs
    width = model // SPLIT
    head_dim = model // HEADS
    hidden = fast_init.shape[0]
    tokens = count * home
    assert tokens == WINDOW // 2 and hidden % (2 * chips) == 0
    rows = hidden // (2 * chips)
    blocks = tokens // LANES
    wide = LANES + WINDOW
    order = frame_order.reshape(count, tok_dev)
    ids = window_ids.reshape(-1, LANES)

    kv, own_q, small = pl.pallas_call(
        functools.partial(pack_kernel, segs),
        name="pack",
        out_shape=(
            jax.ShapeDtypeStruct((SPLIT, segs, 2 * home, width), BF),
            jax.ShapeDtypeStruct((SPLIT, segs, home, width), BF),
            jax.ShapeDtypeStruct((SPLIT, 4, tok_dev), F32),
        ),
        grid=(SPLIT,),
        in_specs=[
            pl.BlockSpec(order.shape, lambda h: (0, 0)),
            pl.BlockSpec((HEADS, tok_dev), lambda h: (0, 0)),
            pl.BlockSpec((tok_dev, width), lambda h: (0, h)),
            pl.BlockSpec((tok_dev, width), lambda h: (0, h)),
            pl.BlockSpec((tok_dev, width), lambda h: (0, h)),
        ],
        out_specs=(
            pl.BlockSpec((1, segs, 2 * home, width), lambda h: (h, 0, 0, 0)),
            pl.BlockSpec((1, segs, home, width), lambda h: (h, 0, 0, 0)),
            pl.BlockSpec((SPLIT, 4, tok_dev), lambda h: (0, 0, 0)),
        ),
        compiler_params=pltpu.CompilerParams(vmem_limit_bytes=16 * 1024 * 1024),
        cost_estimate=pl.CostEstimate(
            flops=6 * tok_dev * tok_dev * model,
            bytes_accessed=12 * tok_dev * model,
            transcendentals=0,
        ),
    )(order, learn_rates.T, queries, key_rows, value_rows)

    dma = pltpu.SemaphoreType.DMA
    return pl.pallas_call(
        functools.partial(layer_kernel, place, head_dim),
        name="layer",
        out_shape=jax.ShapeDtypeStruct((tok_dev, model), BF),
        in_specs=[VM, VM, VM, VM, ANY, VM],
        out_specs=VM,
        scratch_shapes=[
            pltpu.VMEM((3, count, 2 * home, width), BF),
            pltpu.VMEM((count, home, width), BF),
            pltpu.VMEM((count, 4, tok_dev), F32),
            pltpu.VMEM((3, hidden, width), BF),
            pltpu.VMEM((3, hidden, width), F32),
            pltpu.VMEM((3, hidden // 2, width), BF),
            pltpu.VMEM((3, hidden // 2, width), BF),
            pltpu.VMEM((chips, 3, rows, width), BF),
            pltpu.VMEM((chips, 3, rows, width), BF),
            pltpu.VMEM((2 * chips, 3, rows, width), BF),
            pltpu.VMEM((2, 3 * tokens, width), BF),
            pltpu.VMEM((tokens, width), BF),
            pltpu.VMEM((blocks, LANES, wide), F32),
            pltpu.VMEM((tokens, width), F32),
            pltpu.VMEM((SPLIT, tok_dev, width), BF),
            pltpu.VMEM((SPLIT, tok_dev, width), BF),
            dma, dma, dma((count,)), dma, dma, dma, dma, dma, dma, dma, dma,
            dma, dma, dma, dma((chips,)), dma, dma((chips,)), dma, dma,
            dma((SPLIT,)), dma((SPLIT,)),
        ],
        compiler_params=pltpu.CompilerParams(
            vmem_limit_bytes=VMEM_BYTES, collective_id=0, has_side_effects=True
        ),
        cost_estimate=pl.CostEstimate(
            flops=60 * tokens * hidden * width, bytes_accessed=20 * tokens * width,
            transcendentals=0,
        ),
    )(kv, own_q, small, ids, fast_init.transpose(1, 0, 2), norm_gain[None, :])


def solution(mesh):
    rows = P(("groups", "tok"), None)
    return jax.shard_map(
        shards,
        mesh=mesh,
        in_specs=(rows, rows, rows, rows, P("groups"), P("groups"), P(), P()),
        out_specs=rows,
        check_vma=False,
    )
```

```python
import functools

import jax
import jax.numpy as jnp
from jax import lax
from jax.experimental import pallas as pl
from jax.experimental.pallas import tpu as pltpu
from jax.sharding import PartitionSpec as P

HEADS = 8
ATT_DIM = 128
WINDOW = 1024
SPLIT = 4

epsilon = 1e-06
BF = jnp.bfloat16
F32 = jnp.float32
I32 = jnp.int32
LANES = 128
VM = pl.BlockSpec(memory_space=pltpu.VMEM)
ANY = pl.BlockSpec(memory_space=pl.ANY)
NT = (((1,), (1,)), ((), ()))
TN = (((0,), (0,)), ((), ()))
VMEM_BYTES = 62 * 1024 * 1024


def dot_nt(a, b):
    return lax.dot_general(a, b, NT, preferred_element_type=F32)


def dot_tn(a, b):
    return lax.dot_general(a, b, TN, preferred_element_type=F32)


def dot_nn(a, b):
    return jnp.dot(a, b, preferred_element_type=F32)


def iota(shape, dim):
    return lax.broadcasted_iota(I32, shape, dim)


class Place:
    def __init__(self, count):
        self.count = count
        self.segs = count // SPLIT
        self.chips = self.segs // 2

    def shift(self, hd):
        return ((hd % 2) * 2 + hd // 2) % self.chips

    def seg(self, hd, within):
        chip, core = within // 2, within % 2
        if self.chips == 4:
            step = 2 * (chip // 2) + (chip % 2 + chip // 2) % 2
        else:
            step = chip
        return (step - self.shift(hd) + self.chips) % self.chips * 2 + core

    def rank(self, hd, seg):
        pair, core = seg // 2, seg % 2
        step = (pair + self.shift(hd)) % self.chips
        if self.chips == 4:
            chip = 2 * (step // 2) + (step + step // 2) % 2
        else:
            chip = step
        return hd * self.segs + chip * 2 + core


def ranks_of(row, segs):
    tokens = row.shape[1]
    down, across = iota((tokens, tokens), 0), iota((tokens, tokens), 1)
    column = jnp.sum(jnp.where(down == across, row, 0.0), axis=1, keepdims=True)
    span = 1.0 / (SPLIT * tokens)

    def sort_key(place, index):
        return jnp.floor((place + 0.5) * span) * tokens + index.astype(F32)

    key_row = sort_key(row, iota((1, tokens), 1))
    key_column = sort_key(column, iota((tokens, 1), 0))
    rank_row = jnp.sum(jnp.where(key_column < key_row, 1.0, 0.0), axis=0, keepdims=True)
    rank_column = jnp.sum(jnp.where(key_row < key_column, 1.0, 0.0), axis=1, keepdims=True)
    pick = jnp.where(down.astype(F32) == rank_row, 1.0, 0.0).astype(BF)
    put = jnp.where(across.astype(F32) == rank_column, 1.0, 0.0)
    return pick, put, column


def layer_kernel(
    place, head_dim, query_hbm, key_hbm, value_hbm, rate_hbm, order_hbm, ids_hbm, init_ref,
    gain_hbm, out_ref,
    stored, rate_ref, order_ref, ids_ref, gain_ref, kv_ref, q_ref, small_ref, kv, queries, small, weight, total, part, half_in, half, slices, fresh, ahead, sorted_q,
    bias, combined, outgoing, returned,
    load_sem, init_sem, kv_send, kv_recv, q_send, q_recv, small_send, small_recv, next_send, next_recv,
    prev_send, prev_recv, core_send, core_recv, cut_send, cut_recv, share_send, share_recv,
    pass_send, pass_recv, back_send, back_recv,
):
    me = lax.axis_index("tok")
    count, segs, chips = place.count, place.segs, place.chips
    hd, within = me // segs, me % segs
    chip, core = within // 2, within % 2
    seg = place.seg(hd, within)
    home, width = queries.shape[1], queries.shape[2]
    tokens = count * home
    hidden = weight.shape[1]
    side = hidden // 2
    rows = side // chips
    heads = width // head_dim
    partner = me + 1 - 2 * core
    after = place.rank(hd, (seg + 1) % segs)
    before = place.rank(hd, (seg + segs - 1) % segs)

    def remote(src, dst, send, recv, device):
        return pltpu.make_async_remote_copy(
            src_ref=src, dst_ref=dst, send_sem=send, recv_sem=recv,
            device_id={"tok": device}, device_id_type=pl.DeviceIdType.MESH,
        )

    def wait_all(buffer, sem):
        pltpu.make_async_copy(buffer, buffer, sem).wait()

    columns = pl.ds(pl.multiple_of(hd * width, LANES), width)

    loads = [
        pltpu.make_async_copy(source, target, load_sem.at[index])
        for index, (source, target) in enumerate(
            (
                (order_hbm, order_ref), (key_hbm, stored.at[0]), (value_hbm, stored.at[1]),
                (rate_hbm, rate_ref), (query_hbm, stored.at[2]), (ids_hbm, ids_ref),
                (gain_hbm, gain_ref),
            )
        )
    ]
    for copy in loads:
        copy.start()
    load = pltpu.make_async_copy(init_ref.at[:, :, columns], weight, init_sem)
    load.start()
    barrier = pltpu.get_barrier_semaphore()

    def greet(step, carry):
        pl.semaphore_signal(
            barrier, inc=1, device_id={"tok": (me + step) % count},
            device_id_type=pl.DeviceIdType.MESH,
        )
        return carry

    lax.fori_loop(1, count, greet, 0)
    loads[0].wait()
    row = order_ref[pl.ds(me, 1), :].astype(F32)
    pick, put, position = ranks_of(row, segs)
    loads[3].wait()
    rates = jnp.dot(rate_ref[...], put, precision=lax.Precision.HIGHEST)
    position = jnp.sum(put * position, axis=0, keepdims=True)
    for index in range(SPLIT):
        small_ref[index, 0:heads, :] = rates[index * heads : (index + 1) * heads]
        small_ref[index, heads : heads + 1, :] = position
        small_ref[index, heads + 1 :, :] = jnp.zeros_like(small_ref[index, heads + 1 :, :])
    loads[1].wait()
    loads[2].wait()
    for index in range(SPLIT):
        lanes = slice(index * width, (index + 1) * width)
        for which in range(2):
            picked = dot_nn(pick, stored[which, :, lanes]).astype(BF)
            kv_ref[index, :, which * home : (which + 1) * home, :] = picked.reshape(
                segs, home, width
            )
    pl.semaphore_wait(barrier, count - 1)

    pairs = [((hd + 2) % 4, hd), (3 - hd, hd + 1 - 2 * (hd % 2))]

    def send_small(pair, first, last):
        def body(step, carry):
            for plane in pair:
                there = plane * segs + (within + step) % segs
                remote(small_ref.at[plane], small.at[me], small_send, small_recv, there).start()
            return carry

        lax.fori_loop(first, last, body, 0)

    def send_rows(pair, first, last):
        def body(step, carry):
            spot = (within + step) % segs
            for plane in pair:
                there = plane * segs + spot
                where = place.seg(plane, spot)
                remote(
                    kv_ref.at[plane, where], kv.at[1, me], kv_send, kv_recv.at[me], there
                ).start()
            return carry

        lax.fori_loop(first, last, body, 0)

    def send_queries(pair, first, last):
        def body(step, carry):
            spot = (within + step) % segs
            for plane in pair:
                there = plane * segs + spot
                where = place.seg(plane, spot)
                remote(q_ref.at[plane, where], queries.at[me], q_send, q_recv, there).start()
            return carry

        lax.fori_loop(first, last, body, 0)

    def each(action):
        for index, pair in enumerate(pairs):
            if index == 0:
                action(pair[:1], 0, 1)
                action(pair, 1, segs)
            else:
                action(pair, 0, segs)

    each(send_small)
    each(send_rows)

    def forward(block, source):
        remote(block, kv.at[0, source], next_send, next_recv, after).start()
        remote(block, kv.at[2, source], prev_send, prev_recv, before).start()

    loads[4].wait()
    for index in range(SPLIT):
        lanes = slice(index * width, (index + 1) * width)
        picked = dot_nn(pick, stored[2, :, lanes]).astype(BF)
        q_ref[index] = picked.reshape(segs, home, width)
    loads[5].wait()
    loads[6].wait()
    own = kv_ref.at[hd, seg]
    forward(own, me)
    kv[1, me] = kv_ref[hd, seg]
    queries[me] = q_ref[hd, seg]
    small[me] = small_ref[hd]

    def arrive(pair, first, last):
        def body(step, carry):
            for plane in pair:
                source = plane * segs + (within + segs - step) % segs
                block = kv.at[1, source]
                remote(block, block, kv_send, kv_recv.at[source], source).wait_recv()
                forward(block, source)
            return carry

        lax.fori_loop(first, last, body, 0)

    total[...] = jnp.zeros_like(total)

    column = iota((1, width), 1)

    def span(which):
        low = which * head_dim // LANES * LANES
        high = -(-(which + 1) * head_dim // LANES) * LANES
        inside = (column[:, low:high] >= which * head_dim) & (
            column[:, low:high] < (which + 1) * head_dim
        )
        return slice(low, high), inside

    def pick_column(index, base, sources, which):
        lane = iota((home, LANES), 1) == index * home + iota((home, LANES), 0)
        held = small[pl.ds(base, sources), which, :]
        chosen = jnp.where(lane[None], held[:, None, :], 0.0)
        return jnp.sum(chosen, axis=2, keepdims=True).reshape(sources * home, 1)

    def learn(pair):
        group = segs * home
        for which in range(heads):
            lanes, inside = span(which)
            keys, values, rate = (
                jnp.concatenate(parts, axis=0)
                for parts in zip(
                    *(
                        (
                            kv[1, pl.ds(plane * segs, segs), 0:home, lanes].reshape(group, -1),
                            kv[1, pl.ds(plane * segs, segs), home : 2 * home, lanes].reshape(
                                group, -1
                            ),
                            pick_column(seg, plane * segs, segs, which),
                        )
                        for plane in pair
                    )
                )
            )
            key_part = jnp.where(inside, keys.astype(F32), 0.0).astype(BF)
            target = jnp.where(inside, values.astype(F32) * rate, 0.0).astype(BF)
            gate = dot_nt(key_part, weight[0, :, lanes])
            upward = dot_nt(key_part, weight[1, :, lanes])
            backward = dot_nt(target, weight[2, :, lanes])
            sigmoid = jax.nn.sigmoid(gate)
            active = gate * sigmoid
            product = (active * upward).astype(BF)
            delta_gate = (backward * upward * sigmoid * (1.0 + gate * (1.0 - sigmoid))).astype(BF)
            delta_upper = (backward * active).astype(BF)
            total[0, :, lanes] += dot_tn(delta_gate, key_part)
            total[1, :, lanes] += dot_tn(delta_upper, key_part)
            total[2, :, lanes] += dot_tn(product, target)

    arrive(pairs[0][:1], 0, 1)
    arrive(pairs[0], 1, segs // 2)
    arrive(pairs[0], segs // 2, segs)
    wait_all(small.at[pl.ds(0, count - 1)], small_recv)
    load.wait()
    learn(pairs[0])
    each(send_queries)
    arrive(pairs[1], 0, segs // 2)
    arrive(pairs[1], segs // 2, segs)
    learn(pairs[1])

    theirs = pl.ds(pl.multiple_of((1 - core) * side, 16), side)
    part[...] = total[:, theirs, :].astype(BF)
    swap = remote(part, half_in, core_send, core_recv, partner)
    swap.start()
    swap.wait_recv()

    def fold(step, carry):
        spot = (chip + 1 + step) % chips
        mine = pl.ds(pl.multiple_of(core * side + spot * rows, 16), rows)
        theirs = pl.ds(pl.multiple_of(spot * rows, 16), rows)
        half[spot] = (total[:, mine, :] + half_in[:, theirs, :].astype(F32)).astype(BF)

        @pl.when(step < chips - 1)
        def _():
            there = hd * segs + spot * 2 + core
            remote(half.at[spot], slices.at[chip], cut_send, cut_recv.at[chip], there).start()

        return carry

    lax.fori_loop(0, chips, fold, 0)

    wait_all(kv.at[0], next_recv)
    wait_all(kv.at[2], prev_recv)
    wait_all(queries.at[pl.ds(0, count - 1)], q_recv)
    def order_of(index):
        spot = pick_column(index, 0, count, heads)
        down, across = iota((tokens, tokens), 0), iota((tokens, tokens), 1)
        row = jnp.sum(jnp.where(down == across, spot, 0.0), axis=0, keepdims=True)
        return jnp.where((down + index * tokens).astype(F32) == row, 1.0, 0.0).astype(BF)

    for which, index in enumerate(((seg + segs - 1) % segs, seg, (seg + 1) % segs)):
        sort = order_of(index)
        keys = kv[which, :, 0:home, :].reshape(tokens, width)
        values = kv[which, :, home : 2 * home, :].reshape(tokens, width)
        ahead[0, which * tokens : (which + 1) * tokens, :] = dot_nn(sort, keys).astype(BF)
        ahead[1, which * tokens : (which + 1) * tokens, :] = dot_nn(sort, values).astype(BF)
        if which == 1:
            sorted_q[...] = dot_nn(sort, queries[...].reshape(tokens, width)).astype(BF)

    reach = WINDOW // 2
    chunk = LANES
    wide = chunk + 2 * reach
    blocks = tokens // chunk
    id_rows = ids_ref.shape[0]
    down, across = iota((chunk, chunk), 0), iota((chunk, chunk), 1)
    for part_index in range(blocks):
        middle = seg * blocks + part_index
        mine = ids_ref[pl.ds(middle, 1), :]
        mine = jnp.sum(jnp.where(down == across, mine, 0), axis=1, keepdims=True)
        for tile in range(wide // chunk):
            block = middle - reach // chunk + tile
            valid = (block >= 0) & (block < id_rows)
            other = ids_ref[pl.ds((block + id_rows) % id_rows, 1), :]
            other = jnp.where(valid, other, -1)
            distance = down - across + (reach - tile * chunk)
            allowed = (mine == other) & (distance < reach) & (distance > -reach)
            bias[part_index, :, tile * chunk : (tile + 1) * chunk] = jnp.where(
                allowed, 0.0, -1e30
            )

    def attend(head, carry):
        lanes = pl.ds(pl.multiple_of(head * ATT_DIM, LANES), ATT_DIM)
        for part_index in range(blocks):
            begin = part_index * chunk
            query = sorted_q[begin : begin + chunk, lanes]
            keys = ahead[0, begin : begin + wide, lanes]
            values = ahead[1, begin : begin + wide, lanes]
            scores = dot_nt(query, keys) * ATT_DIM ** (-0.5) + bias[part_index]
            peak = jnp.max(scores, axis=1, keepdims=True)
            weights = jnp.exp(scores - peak)
            norm = jnp.sum(weights, axis=1, keepdims=True)
            combined[begin : begin + chunk, lanes] = dot_nn(weights.astype(BF), values) / norm
        return carry

    def cut_arrive(step, carry):
        source = (chip + step) % chips
        block = slices.at[source]
        remote(block, block, cut_send, cut_recv.at[source], me).wait_recv()
        return carry

    early = width // ATT_DIM // 2
    lax.fori_loop(0, early, attend, 0)

    lax.fori_loop(1, chips, cut_arrive, 0)
    slices[chip] = half[chip]
    slot = core * chips + chip
    mine = pl.ds(pl.multiple_of(slot * rows, 16), rows)
    for matrix in range(3):
        base = weight[matrix, mine, :].astype(F32)
        update = base + jnp.sum(slices[:, matrix].astype(F32), axis=0)
        scaling = jnp.zeros_like(update)
        for which in range(heads):
            inside = (column >= which * head_dim) & (column < (which + 1) * head_dim)
            old = jnp.sum(jnp.where(inside, base * base, 0.0), axis=1, keepdims=True)
            new = jnp.sum(jnp.where(inside, update * update, 0.0), axis=1, keepdims=True)
            ratio = jnp.sqrt(old + epsilon) / jnp.sqrt(new + epsilon)
            scaling = jnp.where(inside, ratio, scaling)
        fresh[slot, matrix] = (update * scaling).astype(BF)

    def share(step, carry):
        spot = (chip + step) % chips
        there = hd * segs + spot * 2 + core
        remote(fresh.at[slot], fresh.at[slot], share_send, share_recv.at[chip], there).start()
        return carry

    lax.fori_loop(1, chips, share, 0)

    def hand(index):
        remote(fresh.at[index], fresh.at[index], pass_send, pass_recv, partner).start()

    hand(slot)
    lax.fori_loop(early, width // ATT_DIM, attend, 0)

    def shared(step, carry):
        source = (chip + step) % chips
        block = fresh.at[core * chips + source]
        remote(block, block, share_send, share_recv.at[source], me).wait_recv()
        hand(core * chips + source)
        return carry

    lax.fori_loop(1, chips, shared, 0)
    wait_all(fresh.at[pl.ds(0, chips)], pass_recv)

    for which in range(heads):
        lanes, inside = span(which)
        query = jnp.where(inside, sorted_q[:, lanes].astype(F32), 0.0).astype(BF)

        def matrix_of(matrix):
            return fresh[:, matrix, :, lanes].reshape(hidden, -1)

        gate = dot_nt(query, matrix_of(0))
        upward = dot_nt(query, matrix_of(1))
        product = (gate * jax.nn.sigmoid(gate) * upward).astype(BF)
        combined[:, lanes] += jnp.where(inside, dot_nn(product, matrix_of(2)), 0.0)

    tok_dev = out_ref.shape[0]
    for piece in range(SPLIT):
        there = seg * SPLIT + piece
        outgoing[piece] = combined[piece * tok_dev : (piece + 1) * tok_dev, :].astype(BF)

        @pl.when(there != me)
        def _():
            remote(
                outgoing.at[piece], returned.at[hd], back_send.at[piece], back_recv.at[hd], there
            ).start()

        @pl.when(there == me)
        def _():
            returned[hd] = outgoing[piece]

    for source in range(SPLIT):
        block = returned.at[source]

        @pl.when(place.rank(source, me // SPLIT) != me)
        def _():
            remote(block, block, back_send.at[0], back_recv.at[source], me).wait_recv()

    square = 0.0
    for source in range(SPLIT):
        piece = returned[source].astype(F32)
        square = square + jnp.sum(piece * piece, axis=1, keepdims=True)
    scale = lax.rsqrt(square / (SPLIT * width) + epsilon)
    for source in range(SPLIT):
        lanes = slice(source * width, (source + 1) * width)
        gain = [
            gain_ref[tile : tile + 1, :]
            for tile in range(source * width // LANES, (source + 1) * width // LANES)
        ]
        gain = jnp.concatenate(gain, axis=1)
        out_ref[:, lanes] = (returned[source].astype(F32) * scale * gain).astype(BF)

    wait_all(small.at[pl.ds(0, count - 1)], small_send)
    wait_all(kv.at[1, pl.ds(0, count - 1)], kv_send)
    wait_all(queries.at[pl.ds(0, count - 1)], q_send)
    wait_all(kv.at[0], next_send)
    wait_all(kv.at[2], prev_send)
    swap.wait_send()
    wait_all(slices.at[pl.ds(0, chips - 1)], cut_send)
    wait_all(fresh.at[pl.ds(0, chips - 1)], share_send)
    wait_all(fresh.at[pl.ds(0, chips)], pass_send)
    for piece in range(SPLIT):
        block = outgoing.at[piece]

        @pl.when(seg * SPLIT + piece != me)
        def _():
            remote(block, block, back_send.at[piece], back_recv.at[0], me).wait_send()


def shards(
    queries, key_rows, value_rows, learn_rates, frame_order, window_ids, fast_init, norm_gain
):
    tok_dev, model = queries.shape
    count = lax.axis_size("tok")
    place = Place(count)
    segs, chips = place.segs, place.chips
    assert count % (2 * SPLIT) == 0 and tok_dev % segs == 0
    home = tok_dev // segs
    width = model // SPLIT
    head_dim = model // HEADS
    hidden = fast_init.shape[0]
    tokens = count * home
    assert tokens == WINDOW // 2 and hidden % (2 * chips) == 0
    rows = hidden // (2 * chips)
    blocks = tokens // LANES
    wide = LANES + WINDOW
    order = frame_order.reshape(count, tok_dev)
    ids = window_ids.reshape(-1, LANES)
    gain = norm_gain.reshape(-1, LANES)

    dma = pltpu.SemaphoreType.DMA
    return pl.pallas_call(
        functools.partial(layer_kernel, place, head_dim),
        name="layer",
        out_shape=jax.ShapeDtypeStruct((tok_dev, model), BF),
        in_specs=[ANY] * 8,
        out_specs=VM,
        scratch_shapes=[
            pltpu.VMEM((3, tok_dev, model), BF),
            pltpu.VMEM((HEADS, tok_dev), F32),
            pltpu.VMEM(order.shape, I32),
            pltpu.VMEM(ids.shape, I32),
            pltpu.VMEM(gain.shape, F32),
            pltpu.VMEM((SPLIT, segs, 2 * home, width), BF),
            pltpu.VMEM((SPLIT, segs, home, width), BF),
            pltpu.VMEM((SPLIT, 4, tok_dev), F32),
            pltpu.VMEM((3, count, 2 * home, width), BF),
            pltpu.VMEM((count, home, width), BF),
            pltpu.VMEM((count, 4, tok_dev), F32),
            pltpu.VMEM((3, hidden, width), BF),
            pltpu.VMEM((3, hidden, width), F32),
            pltpu.VMEM((3, hidden // 2, width), BF),
            pltpu.VMEM((3, hidden // 2, width), BF),
            pltpu.VMEM((chips, 3, rows, width), BF),
            pltpu.VMEM((chips, 3, rows, width), BF),
            pltpu.VMEM((2 * chips, 3, rows, width), BF),
            pltpu.VMEM((2, 3 * tokens, width), BF),
            pltpu.VMEM((tokens, width), BF),
            pltpu.VMEM((blocks, LANES, wide), F32),
            pltpu.VMEM((tokens, width), F32),
            pltpu.VMEM((SPLIT, tok_dev, width), BF),
            pltpu.VMEM((SPLIT, tok_dev, width), BF),
            dma((7,)), dma, dma, dma((count,)), dma, dma, dma, dma, dma, dma, dma, dma,
            dma, dma, dma, dma((chips,)), dma, dma((chips,)), dma, dma,
            dma((SPLIT,)), dma((SPLIT,)),
        ],
        compiler_params=pltpu.CompilerParams(
            vmem_limit_bytes=VMEM_BYTES, collective_id=0, has_side_effects=True
        ),
        cost_estimate=pl.CostEstimate(
            flops=60 * tokens * hidden * width, bytes_accessed=20 * tokens * width,
            transcendentals=0,
        ),
    )(
        queries, key_rows, value_rows, learn_rates.T, order, ids,
        fast_init.transpose(1, 0, 2), gain,
    )


def solution(mesh):
    rows = P(("groups", "tok"), None)
    return jax.shard_map(
        shards,
        mesh=mesh,
        in_specs=(rows, rows, rows, rows, P("groups"), P("groups"), P(), P()),
        out_specs=rows,
        check_vma=False,
    )
```

```python
import functools

import jax
import jax.numpy as jnp
from jax import lax
from jax.experimental import pallas as pl
from jax.experimental.pallas import tpu as pltpu
from jax.sharding import PartitionSpec as P

HEADS = 8
ATT_DIM = 128
WINDOW = 1024
SPLIT = 4

epsilon = 1e-06
BF = jnp.bfloat16
F32 = jnp.float32
I32 = jnp.int32
LANES = 128
VM = pl.BlockSpec(memory_space=pltpu.VMEM)
ANY = pl.BlockSpec(memory_space=pl.ANY)
NT = (((1,), (1,)), ((), ()))
TN = (((0,), (0,)), ((), ()))
VMEM_BYTES = 62 * 1024 * 1024


def dot_nt(a, b):
    return lax.dot_general(a, b, NT, preferred_element_type=F32)


def dot_tn(a, b):
    return lax.dot_general(a, b, TN, preferred_element_type=F32)


def dot_nn(a, b):
    return jnp.dot(a, b, preferred_element_type=F32)


def iota(shape, dim):
    return lax.broadcasted_iota(I32, shape, dim)


class Place:
    def __init__(self, count):
        self.count = count
        self.segs = count // SPLIT
        self.chips = self.segs // 2

    def shift(self, hd):
        return ((hd % 2) * 2 + hd // 2) % self.chips

    def seg(self, hd, within):
        chip, core = within // 2, within % 2
        if self.chips == 4:
            step = 2 * (chip // 2) + (chip % 2 + chip // 2) % 2
        else:
            step = chip
        return (step - self.shift(hd) + self.chips) % self.chips * 2 + core

    def rank(self, hd, seg):
        pair, core = seg // 2, seg % 2
        step = (pair + self.shift(hd)) % self.chips
        if self.chips == 4:
            chip = 2 * (step // 2) + (step + step // 2) % 2
        else:
            chip = step
        return hd * self.segs + chip * 2 + core


def ranks_of(row, segs):
    tokens = row.shape[1]
    down, across = iota((tokens, tokens), 0), iota((tokens, tokens), 1)
    column = jnp.sum(jnp.where(down == across, row, 0.0), axis=1, keepdims=True)
    span = 1.0 / (SPLIT * tokens)

    def sort_key(place, index):
        return jnp.floor((place + 0.5) * span) * tokens + index.astype(F32)

    key_row = sort_key(row, iota((1, tokens), 1))
    key_column = sort_key(column, iota((tokens, 1), 0))
    rank_row = jnp.sum(jnp.where(key_column < key_row, 1.0, 0.0), axis=0, keepdims=True)
    rank_column = jnp.sum(jnp.where(key_row < key_column, 1.0, 0.0), axis=1, keepdims=True)
    pick = jnp.where(down.astype(F32) == rank_row, 1.0, 0.0).astype(BF)
    put = jnp.where(across.astype(F32) == rank_column, 1.0, 0.0)
    return pick, put, column


def layer_kernel(
    place, head_dim, query_hbm, key_hbm, value_hbm, rate_hbm, order_hbm, ids_hbm, init_ref,
    gain_hbm, out_ref,
    stored, rate_ref, order_ref, ids_ref, gain_ref, kv_ref, q_ref, small_ref, kv, queries, small, weight, total, part, half_in, half, slices, fresh, ahead, sorted_q,
    bias, combined, products, outgoing, returned,
    load_sem, init_sem, kv_send, kv_recv, q_send, q_recv, small_send, small_recv, next_send, next_recv,
    prev_send, prev_recv, core_send, core_recv, cut_send, cut_recv, relay_send, share_send, share_recv,
    pass_send, pass_recv, back_send, back_recv,
):
    me = lax.axis_index("tok")
    count, segs, chips = place.count, place.segs, place.chips
    hd, within = me // segs, me % segs
    chip, core = within // 2, within % 2
    seg = place.seg(hd, within)
    home, width = queries.shape[1], queries.shape[2]
    tokens = count * home
    hidden = weight.shape[1]
    side = hidden // 2
    rows = side // chips
    heads = width // head_dim
    partner = me + 1 - 2 * core
    after = place.rank(hd, (seg + 1) % segs)
    before = place.rank(hd, (seg + segs - 1) % segs)

    def remote(src, dst, send, recv, device):
        return pltpu.make_async_remote_copy(
            src_ref=src, dst_ref=dst, send_sem=send, recv_sem=recv,
            device_id={"tok": device}, device_id_type=pl.DeviceIdType.MESH,
        )

    def wait_all(buffer, sem):
        pltpu.make_async_copy(buffer, buffer, sem).wait()

    columns = pl.ds(pl.multiple_of(hd * width, LANES), width)

    loads = [
        pltpu.make_async_copy(source, target, load_sem.at[index])
        for index, (source, target) in enumerate(
            (
                (order_hbm, order_ref), (key_hbm, stored.at[0]), (value_hbm, stored.at[1]),
                (rate_hbm, rate_ref), (query_hbm, stored.at[2]), (ids_hbm, ids_ref),
                (gain_hbm, gain_ref),
            )
        )
    ]
    for copy in loads:
        copy.start()
    load = pltpu.make_async_copy(init_ref.at[:, :, columns], weight, init_sem)
    load.start()
    barrier = pltpu.get_barrier_semaphore()

    def greet(step, carry):
        pl.semaphore_signal(
            barrier, inc=1, device_id={"tok": (me + step) % count},
            device_id_type=pl.DeviceIdType.MESH,
        )
        return carry

    lax.fori_loop(1, count, greet, 0)
    loads[0].wait()
    row = order_ref[pl.ds(me, 1), :].astype(F32)
    pick, put, position = ranks_of(row, segs)
    loads[3].wait()
    rates = jnp.dot(rate_ref[...], put, precision=lax.Precision.HIGHEST)
    position = jnp.sum(put * position, axis=0, keepdims=True)
    for index in range(SPLIT):
        small_ref[index, 0:heads, :] = rates[index * heads : (index + 1) * heads]
        small_ref[index, heads : heads + 1, :] = position
        small_ref[index, heads + 1 :, :] = jnp.zeros_like(small_ref[index, heads + 1 :, :])
    loads[1].wait()
    loads[2].wait()
    for index in range(SPLIT):
        lanes = slice(index * width, (index + 1) * width)
        for which in range(2):
            picked = dot_nn(pick, stored[which, :, lanes]).astype(BF)
            kv_ref[index, :, which * home : (which + 1) * home, :] = picked.reshape(
                segs, home, width
            )
    pl.semaphore_wait(barrier, count - 1)

    across, mirror, sibling = (hd + 2) % SPLIT, SPLIT - 1 - hd, hd + 1 - 2 * (hd % 2)
    outer = 1 - (hd + 1) // 2 % 2

    def choose(first, second):
        return second + outer * (first - second)

    ahead_of = (
        (choose(across, hd), choose(mirror, sibling)),
        (choose(hd, across), choose(sibling, mirror)),
    )
    expected = (
        (choose(mirror, across), choose(sibling, hd)),
        (choose(across, mirror), choose(hd, sibling)),
    )

    def send_small(plane, step):
        there = plane * segs + (within + step) % segs
        remote(small_ref.at[plane], small.at[me], small_send, small_recv, there).start()

    def send_rows(plane, step):
        spot = (within + step) % segs
        remote(
            kv_ref.at[plane, place.seg(plane, spot)], kv.at[1, me], kv_send, kv_recv.at[me],
            plane * segs + spot,
        ).start()

    def send_queries(plane, step):
        spot = (within + step) % segs
        remote(
            q_ref.at[plane, place.seg(plane, spot)], queries.at[me], q_send, q_recv,
            plane * segs + spot,
        ).start()

    def others(action, group):
        def body(step, carry):
            for plane in group:

                @pl.when(plane * segs + step != hd * segs)
                def _():
                    action(plane, step)

            return carry

        lax.fori_loop(0, segs, body, 0)

    for action in (send_small, send_rows):
        for group in ahead_of:
            others(action, group)

    def forward(block, source):
        remote(block, kv.at[0, source], next_send, next_recv, after).start()
        remote(block, kv.at[2, source], prev_send, prev_recv, before).start()

    loads[4].wait()
    for index in range(SPLIT):
        lanes = slice(index * width, (index + 1) * width)
        picked = dot_nn(pick, stored[2, :, lanes]).astype(BF)
        q_ref[index] = picked.reshape(segs, home, width)
    loads[5].wait()
    loads[6].wait()
    own = kv_ref.at[hd, seg]
    forward(own, me)
    kv[1, me] = kv_ref[hd, seg]
    queries[me] = q_ref[hd, seg]
    small[me] = small_ref[hd]

    def arrive(plane, step):
        source = plane * segs + (within + segs - step) % segs
        block = kv.at[1, source]
        remote(block, block, kv_send, kv_recv.at[source], source).wait_recv()
        forward(block, source)

    total[...] = jnp.zeros_like(total)

    column = iota((1, width), 1)

    def span(which):
        low = which * head_dim // LANES * LANES
        high = -(-(which + 1) * head_dim // LANES) * LANES
        inside = (column[:, low:high] >= which * head_dim) & (
            column[:, low:high] < (which + 1) * head_dim
        )
        return slice(low, high), inside

    def pick_column(index, base, sources, which):
        lane = iota((home, LANES), 1) == index * home + iota((home, LANES), 0)
        held = small[pl.ds(base, sources), which, :]
        chosen = jnp.where(lane[None], held[:, None, :], 0.0)
        return jnp.sum(chosen, axis=2, keepdims=True).reshape(sources * home, 1)

    theirs = pl.ds(pl.multiple_of((1 - core) * side, 16), side)
    swaps = [
        remote(part.at[m], half_in.at[m], core_send.at[m], core_recv.at[m], partner)
        for m in range(3)
    ]

    def learn(group, swaps):
        sources = [
            plane * segs + (within + segs - step) % segs
            for plane in group
            for step in range(segs)
        ]
        terms = []
        for which in range(heads):
            lanes, inside = span(which)
            keys = jnp.concatenate([kv[1, source, 0:home, lanes] for source in sources], axis=0)
            values = jnp.concatenate(
                [kv[1, source, home : 2 * home, lanes] for source in sources], axis=0
            )
            rate = jnp.concatenate([pick_column(seg, source, 1, which) for source in sources], axis=0)
            key_part = jnp.where(inside, keys.astype(F32), 0.0).astype(BF)
            target = jnp.where(inside, values.astype(F32) * rate, 0.0).astype(BF)
            gate = dot_nt(key_part, weight[0, :, lanes])
            upward = dot_nt(key_part, weight[1, :, lanes])
            backward = dot_nt(target, weight[2, :, lanes])
            sigmoid = jax.nn.sigmoid(gate)
            active = gate * sigmoid
            product = (active * upward).astype(BF)
            delta_gate = (backward * upward * sigmoid * (1.0 + gate * (1.0 - sigmoid))).astype(BF)
            delta_upper = (backward * active).astype(BF)
            terms.append(
                (lanes, (delta_gate, key_part), (delta_upper, key_part), (product, target))
            )
        for matrix in range(3):
            for term in terms:
                left, right = term[1 + matrix]
                total[matrix, :, term[0]] += dot_tn(left, right)
            if swaps:
                part[matrix] = total[matrix, theirs, :].astype(BF)
                swaps[matrix].start()

    reach = WINDOW // 2
    chunk = LANES
    wide = chunk + 2 * reach
    blocks = tokens // chunk
    id_rows = ids_ref.shape[0]
    down, across = iota((chunk, chunk), 0), iota((chunk, chunk), 1)
    for part_index in range(blocks):
        middle = seg * blocks + part_index
        mine = ids_ref[pl.ds(middle, 1), :]
        mine = jnp.sum(jnp.where(down == across, mine, 0), axis=1, keepdims=True)
        for tile in range(wide // chunk):
            block = middle - reach // chunk + tile
            valid = (block >= 0) & (block < id_rows)
            other = ids_ref[pl.ds((block + id_rows) % id_rows, 1), :]
            other = jnp.where(valid, other, -1)
            distance = down - across + (reach - tile * chunk)
            allowed = (mine == other) & (distance < reach) & (distance > -reach)
            bias[part_index, :, tile * chunk : (tile + 1) * chunk] = jnp.where(
                allowed, 0.0, -1e30
            )
    others(arrive, expected[0])
    wait_all(small.at[pl.ds(0, count - 1)], small_recv)
    load.wait()
    learn(expected[0], [])

    def all_queries():
        for group in ahead_of:
            others(send_queries, group)

    pl.when(outer == 0)(all_queries)
    others(arrive, expected[1])
    learn(expected[1], swaps)

    assert chips == 4
    flip, turn, corner = chip + 1 - 2 * (chip % 2), (chip + 2) % chips, chips - 1 - chip
    first_peer = flip + core * (turn - flip)
    second_peer = turn + core * (flip - turn)

    def on(spot):
        return hd * segs + spot * 2 + core

    def fold(matrix):
        def body(spot, carry):
            mine = pl.ds(pl.multiple_of(core * side + spot * rows, 16), rows)
            theirs = pl.ds(pl.multiple_of(spot * rows, 16), rows)
            half[matrix, spot] = (
                total[matrix, mine, :] + half_in[matrix, theirs, :].astype(F32)
            ).astype(BF)
            return carry

        lax.fori_loop(0, chips, body, 0)
        for index, spot in enumerate((corner, first_peer)):
            remote(
                half.at[matrix, spot], slices.at[matrix, index], cut_send,
                cut_recv.at[3 * matrix + index], on(first_peer),
            ).start()

    def landed(matrix, index):
        block = slices.at[matrix, index]
        remote(block, block, cut_send, cut_recv.at[3 * matrix + index], me).wait_recv()

    def relay(matrix):
        landed(matrix, 0)
        slices[matrix, 3] = (
            half[matrix, second_peer].astype(F32) + slices[matrix, 0].astype(F32)
        ).astype(BF)
        remote(
            slices.at[matrix, 3], slices.at[matrix, 2], relay_send, cut_recv.at[3 * matrix + 2],
            on(second_peer),
        ).start()

    for matrix in range(3):
        swaps[matrix].wait_recv()
        fold(matrix)
    def order_of(index):
        spot = pick_column(index, 0, count, heads)
        down, across = iota((tokens, tokens), 0), iota((tokens, tokens), 1)
        row = jnp.sum(jnp.where(down == across, spot, 0.0), axis=0, keepdims=True)
        return jnp.where((down + index * tokens).astype(F32) == row, 1.0, 0.0).astype(BF)

    def arrange(which, index):
        sort = order_of(index)
        keys = kv[which, :, 0:home, :].reshape(tokens, width)
        values = kv[which, :, home : 2 * home, :].reshape(tokens, width)
        ahead[0, which * tokens : (which + 1) * tokens, :] = dot_nn(sort, keys).astype(BF)
        ahead[1, which * tokens : (which + 1) * tokens, :] = dot_nn(sort, values).astype(BF)
        return sort

    slot = core * chips + chip
    mine = pl.ds(pl.multiple_of(slot * rows, 16), rows)

    def hand(matrix, index):
        block = fresh.at[matrix, index]
        remote(block, block, pass_send, pass_recv.at[matrix], partner).start()

    def renew(matrix):
        landed(matrix, 1)
        landed(matrix, 2)
        base = weight[matrix, mine, :].astype(F32)
        update = (
            base
            + half[matrix, chip].astype(F32)
            + slices[matrix, 1].astype(F32)
            + slices[matrix, 2].astype(F32)
        )
        scaling = jnp.zeros_like(update)
        for which in range(heads):
            inside = (column >= which * head_dim) & (column < (which + 1) * head_dim)
            old = jnp.sum(jnp.where(inside, base * base, 0.0), axis=1, keepdims=True)
            new = jnp.sum(jnp.where(inside, update * update, 0.0), axis=1, keepdims=True)
            ratio = jnp.sqrt(old + epsilon) / jnp.sqrt(new + epsilon)
            scaling = jnp.where(inside, ratio, scaling)
        fresh[matrix, slot] = (update * scaling).astype(BF)
        share(matrix, chip, second_peer)
        share(matrix, chip, first_peer)
        hand(matrix, slot)

    def share(matrix, source, peer):
        block = fresh.at[matrix, core * chips + source]
        remote(block, block, share_send, share_recv.at[matrix * chips + source], on(peer)).start()

    def collect(matrix, source):
        block = fresh.at[matrix, core * chips + source]
        remote(block, block, share_send, share_recv.at[matrix * chips + source], me).wait_recv()

    def onward(matrix):
        collect(matrix, second_peer)
        share(matrix, second_peer, first_peer)
        hand(matrix, core * chips + second_peer)

    def gather(matrix):
        for source in (first_peer, corner):
            collect(matrix, source)
            hand(matrix, core * chips + source)

    def whole(matrix, lanes):
        return fresh[matrix, :, :, lanes].reshape(hidden, -1)

    def attend(head, carry):
        lanes = pl.ds(pl.multiple_of(head * ATT_DIM, LANES), ATT_DIM)
        for part_index in range(blocks):
            begin = part_index * chunk
            query = sorted_q[begin : begin + chunk, lanes]
            keys = ahead[0, begin : begin + wide, lanes]
            values = ahead[1, begin : begin + wide, lanes]
            scores = dot_nt(query, keys) * ATT_DIM ** (-0.5) + bias[part_index]
            peak = jnp.max(scores, axis=1, keepdims=True)
            weights = jnp.exp(scores - peak)
            norm = jnp.sum(weights, axis=1, keepdims=True)
            combined[begin : begin + chunk, lanes] = dot_nn(weights.astype(BF), values) / norm
        return carry

    wait_all(kv.at[0], next_recv)
    wait_all(kv.at[2], prev_recv)
    own_order = arrange(1, seg)
    arrange(0, (seg + segs - 1) % segs)
    for matrix in range(3):
        relay(matrix)
    pl.when(outer == 1)(all_queries)
    arrange(2, (seg + 1) % segs)
    attend_heads = width // ATT_DIM
    first = max(attend_heads - 4, 0)
    renew(0)
    renew(1)
    renew(2)
    wait_all(queries.at[pl.ds(0, count - 1)], q_recv)
    sorted_q[...] = dot_nn(own_order, queries[...].reshape(tokens, width)).astype(BF)
    lax.fori_loop(0, first, attend, 0)
    onward(0)
    onward(1)
    onward(2)
    lax.fori_loop(first, first + 2, attend, 0)
    gather(0)
    lax.fori_loop(first + 2, first + 3, attend, 0)
    gather(1)
    lax.fori_loop(first + 3, attend_heads, attend, 0)
    wait_all(fresh.at[0, pl.ds(0, chips)], pass_recv.at[0])
    wait_all(fresh.at[1, pl.ds(0, chips)], pass_recv.at[1])
    for which in range(heads):
        lanes, inside = span(which)
        query = jnp.where(inside, sorted_q[:, lanes].astype(F32), 0.0).astype(BF)
        gate = dot_nt(query, whole(0, lanes))
        upward = dot_nt(query, whole(1, lanes))
        products[which] = (gate * jax.nn.sigmoid(gate) * upward).astype(BF)
    gather(2)
    wait_all(fresh.at[2, pl.ds(0, chips)], pass_recv.at[2])
    tok_dev = out_ref.shape[0]
    for step in range(SPLIT):
        piece = (within + hd + step) % SPLIT
        there = seg * SPLIT + piece
        stretch = pl.ds(pl.multiple_of(piece * tok_dev, tok_dev), tok_dev)
        for which in range(heads):
            lanes, inside = span(which)
            made = dot_nn(products[which, stretch, :], whole(2, lanes))
            combined[stretch, lanes] += jnp.where(inside, made, 0.0)
        outgoing[piece] = combined[stretch, :].astype(BF)

        @pl.when(there != me)
        def _():
            remote(
                outgoing.at[piece], returned.at[hd], back_send.at[piece], back_recv.at[hd], there
            ).start()

        @pl.when(there == me)
        def _():
            returned[hd] = outgoing[piece]

    for source in range(SPLIT):
        block = returned.at[source]

        @pl.when(place.rank(source, me // SPLIT) != me)
        def _():
            remote(block, block, back_send.at[0], back_recv.at[source], me).wait_recv()

    square = 0.0
    for source in range(SPLIT):
        piece = returned[source].astype(F32)
        square = square + jnp.sum(piece * piece, axis=1, keepdims=True)
    scale = lax.rsqrt(square / (SPLIT * width) + epsilon)
    for source in range(SPLIT):
        lanes = slice(source * width, (source + 1) * width)
        gain = [
            gain_ref[tile : tile + 1, :]
            for tile in range(source * width // LANES, (source + 1) * width // LANES)
        ]
        gain = jnp.concatenate(gain, axis=1)
        out_ref[:, lanes] = (returned[source].astype(F32) * scale * gain).astype(BF)

    wait_all(small.at[pl.ds(0, count - 1)], small_send)
    wait_all(kv.at[1, pl.ds(0, count - 1)], kv_send)
    wait_all(queries.at[pl.ds(0, count - 1)], q_send)
    wait_all(kv.at[0], next_send)
    wait_all(kv.at[2], prev_send)
    for matrix in range(3):
        swaps[matrix].wait_send()
    wait_all(slices.at[:, pl.ds(0, 2)], cut_send)
    wait_all(slices.at[:, 3], relay_send)
    wait_all(fresh.at[:, pl.ds(0, chips - 1)], share_send)
    wait_all(fresh.at[:, pl.ds(0, chips)], pass_send)
    for piece in range(SPLIT):
        block = outgoing.at[piece]

        @pl.when(seg * SPLIT + piece != me)
        def _():
            remote(block, block, back_send.at[piece], back_recv.at[0], me).wait_send()


def shards(
    queries, key_rows, value_rows, learn_rates, frame_order, window_ids, fast_init, norm_gain
):
    tok_dev, model = queries.shape
    count = lax.axis_size("tok")
    place = Place(count)
    segs, chips = place.segs, place.chips
    assert count % (2 * SPLIT) == 0 and tok_dev % segs == 0
    home = tok_dev // segs
    width = model // SPLIT
    head_dim = model // HEADS
    hidden = fast_init.shape[0]
    tokens = count * home
    assert tokens == WINDOW // 2 and hidden % (2 * chips) == 0
    rows = hidden // (2 * chips)
    blocks = tokens // LANES
    wide = LANES + WINDOW
    order = frame_order.reshape(count, tok_dev)
    ids = window_ids.reshape(-1, LANES)
    gain = norm_gain.reshape(-1, LANES)

    dma = pltpu.SemaphoreType.DMA
    return pl.pallas_call(
        functools.partial(layer_kernel, place, head_dim),
        name="layer",
        out_shape=jax.ShapeDtypeStruct((tok_dev, model), BF),
        in_specs=[ANY] * 8,
        out_specs=VM,
        scratch_shapes=[
            pltpu.VMEM((3, tok_dev, model), BF),
            pltpu.VMEM((HEADS, tok_dev), F32),
            pltpu.VMEM(order.shape, I32),
            pltpu.VMEM(ids.shape, I32),
            pltpu.VMEM(gain.shape, F32),
            pltpu.VMEM((SPLIT, segs, 2 * home, width), BF),
            pltpu.VMEM((SPLIT, segs, home, width), BF),
            pltpu.VMEM((SPLIT, 4, tok_dev), F32),
            pltpu.VMEM((3, count, 2 * home, width), BF),
            pltpu.VMEM((count, home, width), BF),
            pltpu.VMEM((count, 4, tok_dev), F32),
            pltpu.VMEM((3, hidden, width), BF),
            pltpu.VMEM((3, hidden, width), F32),
            pltpu.VMEM((3, hidden // 2, width), BF),
            pltpu.VMEM((3, hidden // 2, width), BF),
            pltpu.VMEM((3, chips, rows, width), BF),
            pltpu.VMEM((3, chips, rows, width), BF),
            pltpu.VMEM((3, 2 * chips, rows, width), BF),
            pltpu.VMEM((2, 3 * tokens, width), BF),
            pltpu.VMEM((tokens, width), BF),
            pltpu.VMEM((blocks, LANES, wide), F32),
            pltpu.VMEM((tokens, width), F32),
            pltpu.VMEM((HEADS // SPLIT, tokens, hidden), BF),
            pltpu.VMEM((SPLIT, tok_dev, width), BF),
            pltpu.VMEM((SPLIT, tok_dev, width), BF),
            dma((7,)), dma, dma, dma((count,)), dma, dma, dma, dma, dma, dma, dma, dma,
            dma((3,)), dma((3,)), dma, dma((9,)), dma, dma,
            dma((3 * chips,)), dma, dma((3,)),
            dma((SPLIT,)), dma((SPLIT,)),
        ],
        compiler_params=pltpu.CompilerParams(
            vmem_limit_bytes=VMEM_BYTES, collective_id=0, has_side_effects=True
        ),
        cost_estimate=pl.CostEstimate(
            flops=60 * tokens * hidden * width, bytes_accessed=20 * tokens * width,
            transcendentals=0,
        ),
    )(
        queries, key_rows, value_rows, learn_rates.T, order, ids,
        fast_init.transpose(1, 0, 2), gain,
    )


def solution(mesh):
    rows = P(("groups", "tok"), None)
    return jax.shard_map(
        shards,
        mesh=mesh,
        in_specs=(rows, rows, rows, rows, P("groups"), P("groups"), P(), P()),
        out_specs=rows,
        check_vma=False,
    )
```
